32 devices in a mesh: tm: 16 (over z, x, core), freq: 2 (over y).
Axes of the slice: x: 2, y: 2, z: 4, core: 2. Of those that a mesh axis runs over, the one named last changes fastest.
Arguments:
- strengths: bfloat16 [2, 8, 256, 32768], P(None, 'freq', None, 'tm'), may hold values from -6 to 6
- sample_cell: int32 [32768], P('tm'), may hold values from 0 to 16383, as said below
- sample_frac: float32 [32768], P('tm'), may hold values from 0 to 1
Outputs:
- spectra: float32 [2, 8, 256, 4, 32, 128], P(None, None, 'tm', 'freq')
The draws below stay inside these ranges and needn't reach their ends.
Inputs may be any that keep to these rules, and one draw needn't show every extreme that they name: `sample_cell`: the samples of the i-th aligned block of 2048 samples lie in cells i * 1024 to (i + 1) * 1024 - 1; in every block the first sample lies in the first of these cells and the second sample in the last.
All inputs are finite; a program needn't handle non-finite values.
Results may differ from the reference program's by a relative error of at most 0.0037.
Values may be sent and summed in bfloat16 or wider, within the bound.
A program may use at most 128 MiB of HBM per device.

```python
import math
import jax
import jax.numpy as jnp
from jax import lax

TAPS = 8
FGROUPS = 8
CHG = 256
GRID_DEV = 1024
SAMP_DEV = 2048
FFT_LO = 32
FFT_HI = 128
FFTLEN = 4096
SAMPLES = 32768
CELLS = 16384
FRAMES = 4


def draw_sample_cell(key, part):
    offsets = jax.random.randint(key, (SAMPLES,), 0, GRID_DEV)
    within = jnp.arange(SAMPLES) % SAMP_DEV
    offsets = jnp.where(within == 0, 0, jnp.where(within == 1, GRID_DEV - 1, offsets))
    blocks = jnp.arange(SAMPLES) // SAMP_DEV
    return (blocks * GRID_DEV + offsets).astype(jnp.int32)


def levels(rng, dims, cuts, least, largest):
    gain, own = 1.0, jax.random.fold_in(rng, 6)
    for dim, blocks in cuts:
        heights = jnp.exp(jax.random.uniform(jax.random.fold_in(own, dim), (blocks,), jnp.float32, least / len(cuts), largest / len(cuts)))
        gain = gain * jnp.repeat(heights, dims[dim] // blocks).reshape([-1 if axis == dim else 1 for axis in range(len(dims))])
    return gain


def scatter_about(key, dims, scale, reach, shards=(), dtype=jnp.bfloat16):
    factor_of = levels(key, dims, shards, -0.22, 0.18) if shards else 1.0
    drawn = jax.random.normal(key, dims, jnp.float32) * scale * factor_of
    return jnp.minimum(jnp.maximum(drawn, -reach), reach).astype(dtype)


def setup_inputs(seed: int = 0) -> dict:
    splits = jax.random.split(jax.random.key(seed), 4)
    return {
        "strengths": scatter_about(splits[0], (2, FGROUPS, CHG, SAMPLES), 1.0, 6.0, ((1, 2), (3, 16))),
        "sample_cell": draw_sample_cell(jax.random.fold_in(splits[3], 71), 0),
        "sample_frac": jnp.clip(1.0 * jax.random.uniform(splits[2], (SAMPLES,), jnp.float32) ** levels(splits[2], (SAMPLES,), ((0, 16),), -0.2, 0.2), 0.0, 1.0),
    }


sharpness = 0.3

def one_group(group_strengths, sample_cell, sample_frac):
    values = group_strengths.astype(jnp.float32)
    accumulated = jnp.zeros((2, CHG, CELLS), jnp.float32)
    for tap_index in range(TAPS):
        shifted = jnp.float32(tap_index) - float(TAPS // 2 - 1) - sample_frac
        weight_row = lax.optimization_barrier(jnp.exp(-sharpness * (shifted * shifted)).astype(jnp.bfloat16)).astype(jnp.float32)
        target = ((sample_cell + (tap_index - (TAPS // 2 - 1))) % CELLS).astype(jnp.int32)
        accumulated = accumulated.at[:, :, target].add(values * weight_row)
    rounded = lax.optimization_barrier(accumulated.astype(jnp.bfloat16)).astype(jnp.float32)
    framed = rounded.reshape(2, CHG, FRAMES, FFTLEN)
    transform = jnp.fft.fft(framed[0] + 1j * framed[1], axis=-1) * (1.0 / math.sqrt(FFTLEN))
    parts = jnp.stack([jnp.real(transform), jnp.imag(transform)]).astype(jnp.float32)
    digits = parts.reshape(2, CHG, FRAMES, FFT_HI, FFT_LO)
    return jnp.swapaxes(digits, -1, -2)

def reference(strengths, sample_cell, sample_frac):
    by_group = jnp.moveaxis(strengths, 1, 0)
    result = lax.map(lambda group_strengths: one_group(group_strengths, sample_cell, sample_frac), by_group)
    return jnp.moveaxis(result, 0, 1)
```

```python
import math

import jax
import jax.numpy as jnp
import numpy as np
from jax import lax
from jax.experimental import pallas as pl
from jax.experimental.pallas import tpu as pltpu
from jax.sharding import PartitionSpec as P

TAPS = 8
HALF = TAPS // 2
GRID_DEV = 1024
FFT_LO = 32
FFT_HI = 128
FFTLEN = 4096
SHARP = 0.3
MESH = pl.DeviceIdType.MESH
SLABS = GRID_DEV // FFT_HI
PER_FRAME = FFTLEN // GRID_DEV


def tap_table(local_cell, fraction, columns):
    offset = columns[None, :] - local_cell[:, None] - 1
    inside = (offset >= 0) & (offset < TAPS)
    shifted = offset.astype(jnp.float32) - float(HALF - 1) - fraction[:, None]
    values = jnp.exp(-SHARP * (shifted * shifted))
    return jnp.where(inside, values, 0.0).astype(jnp.bfloat16)


def spread_kernel(s_ref, h_ref, w_ref, e_ref, o_ref):
    rows = s_ref.shape[0] * s_ref.shape[1] * s_ref.shape[2]
    s = s_ref[...].reshape(rows, s_ref.shape[3])
    h = h_ref[...].reshape(rows, h_ref.shape[3])
    acc = jnp.dot(s, w_ref[...], preferred_element_type=jnp.float32)
    acc = acc + jnp.dot(h, e_ref[...], preferred_element_type=jnp.float32)
    acc = acc.astype(jnp.bfloat16)
    for j in range(SLABS):
        o_ref[0, j] = acc[:, j * FFT_HI : (j + 1) * FFT_HI]


def spread(strengths, halo_cols, table, select, n_tm):
    parts, groups, channels, samples = strengths.shape
    chunk = channels // n_tm
    rows = parts * groups * chunk
    lanes = halo_cols.shape[3]
    return pl.pallas_call(
        spread_kernel,
        out_shape=jax.ShapeDtypeStruct((n_tm, SLABS, rows, FFT_HI), jnp.bfloat16),
        grid=(n_tm,),
        in_specs=[
            pl.BlockSpec((parts, groups, chunk, samples), lambda d: (0, 0, d, 0)),
            pl.BlockSpec((parts, groups, chunk, lanes), lambda d: (0, 0, d, 0)),
            pl.BlockSpec((samples, GRID_DEV), lambda d: (0, 0)),
            pl.BlockSpec((lanes, GRID_DEV), lambda d: (0, 0)),
        ],
        out_specs=pl.BlockSpec((1, SLABS, rows, FFT_HI), lambda d: (d, 0, 0, 0)),
        name="spread",
    )(strengths, halo_cols, table, select)


def exchange_kernel(n_tm, n_fq, src, out, send1, recv1, send2, recv2, local_sem):
    t = lax.axis_index("tm")
    f = lax.axis_index("freq")
    span = n_tm // n_fq
    slot = lax.rem(t, span)
    home = lax.div(t, span)
    barrier = pltpu.get_barrier_semaphore()

    def greet_tm(i, c):
        pl.semaphore_signal(barrier, inc=1, device_id=(lax.rem(t + i, n_tm), f), device_id_type=MESH)
        return c

    def greet_fq(i, c):
        pl.semaphore_signal(barrier, inc=1, device_id=(t, lax.rem(f + i, n_fq)), device_id_type=MESH)
        return c

    lax.fori_loop(1, n_tm, greet_tm, 0)
    lax.fori_loop(1, n_fq, greet_fq, 0)
    pl.semaphore_wait(barrier, n_tm - 1 + n_fq - 1)

    def place(target):
        return jnp.where(target == f, f, n_fq + target)

    def first(peer):
        return pltpu.make_async_remote_copy(
            src_ref=src.at[peer],
            dst_ref=out.at[place(home), slot],
            send_sem=send1.at[peer],
            recv_sem=recv1.at[t],
            device_id=(peer, f),
            device_id_type=MESH,
        )

    def first_landed(origin):
        return pltpu.make_async_remote_copy(
            src_ref=src.at[origin],
            dst_ref=out.at[place(lax.div(origin, span)), lax.rem(origin, span)],
            send_sem=send1.at[origin],
            recv_sem=recv1.at[origin],
            device_id=(origin, f),
            device_id_type=MESH,
        )

    def second(target, s):
        return pltpu.make_async_remote_copy(
            src_ref=out.at[n_fq + target, s],
            dst_ref=out.at[f, s],
            send_sem=send2.at[target, s],
            recv_sem=recv2.at[f, s],
            device_id=(t, target),
            device_id_type=MESH,
        )

    def second_landed(origin, s):
        return pltpu.make_async_remote_copy(
            src_ref=out.at[n_fq + origin, s],
            dst_ref=out.at[origin, s],
            send_sem=send2.at[origin, s],
            recv_sem=recv2.at[origin, s],
            device_id=(t, origin),
            device_id_type=MESH,
        )

    half = n_tm // 2
    upper = lax.div(t, half)

    def far(i, c):
        first((1 - upper) * half + lax.rem(t + i, half)).start()
        return c

    def near(i, c):
        first(upper * half + lax.rem(t + i, half)).start()
        return c

    lax.fori_loop(0, half, far, 0)
    lax.fori_loop(1, half, near, 0)
    own = pltpu.make_async_copy(src.at[t], out.at[place(home), slot], local_sem)
    own.start()
    own.wait()

    def relay_group(k, c):
        target = lax.rem(f + k, n_fq)

        def relay(i, c):
            s = lax.rem(slot + span - i, span)
            origin = target * span + s

            @pl.when(origin != t)
            def _():
                first_landed(origin).wait_recv()

            second(target, s).start()
            return c

        return lax.fori_loop(0, span, relay, c)

    lax.fori_loop(1, n_fq, relay_group, 0)

    def kept(s, c):
        origin = f * span + s

        @pl.when(origin != t)
        def _():
            first_landed(origin).wait_recv()

        return c

    lax.fori_loop(0, span, kept, 0)

    def finish_first(i, c):
        first(lax.rem(t + i, n_tm)).wait_send()
        return c

    lax.fori_loop(1, n_tm, finish_first, 0)

    def finish_group(k, c):
        other = lax.rem(f + k, n_fq)

        def finish(s, c):
            second(other, s).wait_send()
            second_landed(other, s).wait_recv()
            return c

        return lax.fori_loop(0, span, finish, c)

    lax.fori_loop(1, n_fq, finish_group, 0)


def exchange(blocks, n_tm, n_fq):
    import functools

    span = n_tm // n_fq
    return pl.pallas_call(
        functools.partial(exchange_kernel, n_tm, n_fq),
        out_shape=jax.ShapeDtypeStruct((2 * n_fq, span) + blocks.shape[1:], jnp.bfloat16),
        in_specs=[pl.BlockSpec(memory_space=pl.ANY)],
        out_specs=pl.BlockSpec(memory_space=pl.ANY),
        scratch_shapes=[
            pltpu.SemaphoreType.DMA((n_tm,)),
            pltpu.SemaphoreType.DMA((n_tm,)),
            pltpu.SemaphoreType.DMA((n_fq, span)),
            pltpu.SemaphoreType.DMA((n_fq, span)),
            pltpu.SemaphoreType.DMA,
        ],
        compiler_params=pltpu.CompilerParams(collective_id=0, has_side_effects=True),
        name="exchange",
    )(blocks)


def fft_list(re, im):
    n = len(re)
    if n == 1:
        return re, im
    er, ei = fft_list(re[0::2], im[0::2])
    orr, oi = fft_list(re[1::2], im[1::2])
    out_r, out_i = [None] * n, [None] * n
    for k in range(n // 2):
        c, s = math.cos(2 * math.pi * k / n), math.sin(2 * math.pi * k / n)
        a, b = orr[k], oi[k]
        if k == 0:
            tr, ti = a, b
        elif 4 * k == n:
            tr, ti = b, -a
        elif 8 * k == n:
            tr, ti = (a + b) * c, (b - a) * c
        elif 8 * k == 3 * n:
            tr, ti = (b - a) * s, -(a + b) * s
        else:
            tr, ti = a * c + b * s, b * c - a * s
        out_r[k], out_i[k] = er[k] + tr, ei[k] + ti
        out_r[k + n // 2], out_i[k + n // 2] = er[k] - tr, ei[k] - ti
    return out_r, out_i


def transform_kernel(x_ref, tc_ref, ts_ref, hi_ref, lo_ref, o_ref, lhs, turned):
    chunk = x_ref.shape[5]
    re = [x_ref[0, n // SLABS, n % SLABS, 0, 0].astype(jnp.float32) for n in range(FFT_LO)]
    im = [x_ref[0, n // SLABS, n % SLABS, 1, 0].astype(jnp.float32) for n in range(FFT_LO)]
    re, im = fft_list(re, im)
    for a in range(FFT_LO):
        c = tc_ref[a : a + 1, :]
        s = ts_ref[a : a + 1, :]
        rows = pl.ds(a * chunk, chunk)
        lhs[rows, :FFT_HI] = (re[a] * c + im[a] * s).astype(jnp.bfloat16)
        lhs[rows, FFT_HI:] = (im[a] * c - re[a] * s).astype(jnp.bfloat16)
    x = lhs[...]
    y = jnp.dot(x, hi_ref[...], preferred_element_type=jnp.float32)
    y = y + jnp.dot(x, lo_ref[...], preferred_element_type=jnp.float32)
    for p in range(2):
        for a in range(FFT_LO):
            turned[p, pl.ds(a, chunk, stride=FFT_LO), :] = y[
                a * chunk : (a + 1) * chunk, p * FFT_HI : (p + 1) * FFT_HI
            ]
        o_ref[p, 0, :, 0] = turned[p].reshape(chunk, FFT_LO, FFT_HI)


def transform(held, n_fq, groups, chunk, frames):
    span = held.shape[1]
    x = held.reshape(2 * n_fq, span, SLABS, 2, groups, chunk, FFT_HI)
    low = np.arange(FFT_LO)[:, None] * np.arange(FFT_HI)[None, :] * (2 * math.pi / FFTLEN)
    high = np.arange(FFT_HI)[:, None] * np.arange(FFT_HI)[None, :] % FFT_HI * (2 * math.pi / FFT_HI)
    hc, hs = np.cos(high), np.sin(high)
    full = np.block([[hc, -hs], [hs, hc]]).astype(np.float32) / math.sqrt(FFTLEN)
    hi = full.astype(jnp.bfloat16)
    lo = (full - hi.astype(np.float32)).astype(jnp.bfloat16)
    whole = lambda shape: pl.BlockSpec(shape, lambda f, g, m: (0, 0))
    return pl.pallas_call(
        transform_kernel,
        out_shape=jax.ShapeDtypeStruct(
            (2, n_fq * groups, chunk, frames, FFT_LO, FFT_HI), jnp.float32
        ),
        grid=(n_fq, groups, frames),
        in_specs=[
            pl.BlockSpec(
                (1, PER_FRAME, SLABS, 2, 1, chunk, FFT_HI), lambda f, g, m: (f, m, 0, 0, g, 0, 0)
            ),
            whole((FFT_LO, FFT_HI)),
            whole((FFT_LO, FFT_HI)),
            whole((2 * FFT_HI, 2 * FFT_HI)),
            whole((2 * FFT_HI, 2 * FFT_HI)),
        ],
        out_specs=pl.BlockSpec(
            (2, 1, chunk, 1, FFT_LO, FFT_HI), lambda f, g, m: (0, f * groups + g, 0, m, 0, 0)
        ),
        scratch_shapes=[
            pltpu.VMEM((FFT_LO * chunk, 2 * FFT_HI), jnp.bfloat16),
            pltpu.VMEM((2, FFT_LO * chunk, FFT_HI), jnp.float32),
        ],
        name="transform",
    )(
        x,
        jnp.asarray(np.cos(low), jnp.float32),
        jnp.asarray(np.sin(low), jnp.float32),
        jnp.asarray(hi),
        jnp.asarray(lo),
    )


def shards(strengths, sample_cell, sample_frac):
    n_tm, n_fq = lax.axis_size("tm"), lax.axis_size("freq")
    parts, groups, channels, samples = strengths.shape
    local_cell = sample_cell - lax.axis_index("tm") * GRID_DEV
    edge_columns = jnp.concatenate(
        [
            jnp.arange(HALF, dtype=jnp.int32),
            jnp.arange(GRID_DEV + HALF, GRID_DEV + TAPS, dtype=jnp.int32),
        ]
    )
    edge_table = tap_table(local_cell, sample_frac, edge_columns)
    edges = lax.dot_general(
        edge_table,
        strengths.reshape(parts * groups * channels, samples),
        (((0,), (1,)), ((), ())),
        preferred_element_type=jnp.float32,
    )
    from_left = lax.ppermute(edges[HALF:], "tm", [(i, (i + 1) % n_tm) for i in range(n_tm)])
    from_right = lax.ppermute(edges[:HALF], "tm", [((i + 1) % n_tm, i) for i in range(n_tm)])
    table = tap_table(local_cell, sample_frac, jnp.arange(HALF, HALF + GRID_DEV, dtype=jnp.int32))
    halo = jnp.concatenate([from_left, from_right], axis=0)
    h0 = lax.reduce_precision(halo, 8, 7)
    h1 = lax.reduce_precision(halo - h0, 8, 7)
    h2 = halo - h0 - h1
    split = jnp.concatenate([h0, h1, h2], axis=0)
    halo_cols = jnp.pad(split.T, ((0, 0), (0, 128 - 3 * TAPS))).astype(jnp.bfloat16)
    pick = np.zeros((128, GRID_DEV), np.float32)
    for r in range(3):
        for k in range(HALF):
            pick[r * TAPS + k, k] = 1.0
            pick[r * TAPS + HALF + k, GRID_DEV - HALF + k] = 1.0
    blocks = spread(
        strengths,
        halo_cols.reshape(parts, groups, channels, 128),
        table,
        jnp.asarray(pick, jnp.bfloat16),
        n_tm,
    )
    held = exchange(blocks, n_tm, n_fq)
    frames = n_tm // PER_FRAME // n_fq
    return transform(held, n_fq, groups, channels // n_tm, frames)


def solution(mesh):
    placed = (P(None, "freq", None, "tm"), P("tm"), P("tm"))
    return jax.shard_map(
        shards,
        mesh=mesh,
        in_specs=placed,
        out_specs=P(None, None, "tm", "freq", None, None),
        check_vma=False,
    )
```

```python
import functools
import math

import jax
import jax.numpy as jnp
import numpy as np
from jax import lax
from jax.experimental import pallas as pl
from jax.experimental.pallas import tpu as pltpu
from jax.sharding import PartitionSpec as P

TAPS = 8
HALF = TAPS // 2
GRID_DEV = 1024
FFT_LO = 32
FFT_HI = 128
FFTLEN = 4096
SHARP = 0.3
MESH = pl.DeviceIdType.MESH
SLABS = GRID_DEV // FFT_HI
PER_FRAME = FFTLEN // GRID_DEV


def tap_table(local_cell, fraction, columns):
    offset = columns[None, :] - local_cell[:, None] - 1
    inside = (offset >= 0) & (offset < TAPS)
    shifted = offset.astype(jnp.float32) - float(HALF - 1) - fraction[:, None]
    values = jnp.exp(-SHARP * (shifted * shifted))
    return jnp.where(inside, values, 0.0).astype(jnp.bfloat16)


def exchange_kernel(
    n_tm, n_fq, strengths, halo, table, select, out, held, src, load, send1, recv1, send2, recv2, local_sem
):
    t = lax.axis_index("tm")
    f = lax.axis_index("freq")
    span = n_tm // n_fq
    slot = lax.rem(t, span)
    home = lax.div(t, span)
    barrier = pltpu.get_barrier_semaphore()

    def greet_tm(i, c):
        pl.semaphore_signal(barrier, inc=1, device_id=(lax.rem(t + i, n_tm), f), device_id_type=MESH)
        return c

    def greet_fq(i, c):
        pl.semaphore_signal(barrier, inc=1, device_id=(t, lax.rem(f + i, n_fq)), device_id_type=MESH)
        return c

    lax.fori_loop(1, n_tm, greet_tm, 0)
    lax.fori_loop(1, n_fq, greet_fq, 0)
    half = n_tm // 2
    upper = lax.div(t, half)
    chunk = held.shape[3]
    rows = src.shape[2]

    def dest(i):
        side = jnp.where(i < half, 1 - upper, upper)
        return side * half + lax.rem(t + 1 + i, half)

    def fetch(i):
        channels = pl.ds(pl.multiple_of(dest(i) * chunk, chunk), chunk)
        return pltpu.make_async_copy(strengths.at[:, :, channels, :], held.at[i], load.at[i])

    def fetch_one(i, c):
        fetch(i).start()
        return c

    lax.fori_loop(0, n_tm, fetch_one, 0)

    def make(i):
        fetch(i).wait()
        channels = pl.ds(pl.multiple_of(dest(i) * chunk, chunk), chunk)
        x = held[i].reshape(rows, held.shape[4])
        h = halo[:, :, channels, :].reshape(rows, halo.shape[3])
        acc = jnp.dot(x, table[...], preferred_element_type=jnp.float32)
        acc = acc + jnp.dot(h, select[...], preferred_element_type=jnp.float32)
        acc = acc.astype(jnp.bfloat16)
        for j in range(SLABS):
            src[dest(i), j] = acc[:, j * FFT_HI : (j + 1) * FFT_HI]

    make(0)
    pl.semaphore_wait(barrier, n_tm - 1 + n_fq - 1)

    def place(target):
        return jnp.where(target == f, f, n_fq + target)

    def first(peer):
        return pltpu.make_async_remote_copy(
            src_ref=src.at[peer],
            dst_ref=out.at[place(home), slot],
            send_sem=send1.at[peer],
            recv_sem=recv1.at[t],
            device_id=(peer, f),
            device_id_type=MESH,
        )

    def first_landed(origin):
        return pltpu.make_async_remote_copy(
            src_ref=src.at[origin],
            dst_ref=out.at[place(lax.div(origin, span)), lax.rem(origin, span)],
            send_sem=send1.at[origin],
            recv_sem=recv1.at[origin],
            device_id=(origin, f),
            device_id_type=MESH,
        )

    def second(target, s):
        return pltpu.make_async_remote_copy(
            src_ref=out.at[n_fq + target, s],
            dst_ref=out.at[f, s],
            send_sem=send2.at[target, s],
            recv_sem=recv2.at[f, s],
            device_id=(t, target),
            device_id_type=MESH,
        )

    def second_landed(origin, s):
        return pltpu.make_async_remote_copy(
            src_ref=out.at[n_fq + origin, s],
            dst_ref=out.at[origin, s],
            send_sem=send2.at[origin, s],
            recv_sem=recv2.at[origin, s],
            device_id=(t, origin),
            device_id_type=MESH,
        )

    def step(i, c):
        make(i)
        first(dest(i - 1)).start()
        return c

    lax.fori_loop(1, n_tm, step, 0)
    own = pltpu.make_async_copy(src.at[t], out.at[place(home), slot], local_sem)
    own.start()
    own.wait()

    def relay_group(k, c):
        target = lax.rem(f + k, n_fq)

        def relay(i, c):
            s = lax.rem(slot + 2 * span - 1 - i, span)
            origin = target * span + s

            @pl.when(origin != t)
            def _():
                first_landed(origin).wait_recv()

            second(target, s).start()
            return c

        return lax.fori_loop(0, span, relay, c)

    lax.fori_loop(1, n_fq, relay_group, 0)

    def kept(s, c):
        origin = f * span + s

        @pl.when(origin != t)
        def _():
            first_landed(origin).wait_recv()

        return c

    lax.fori_loop(0, span, kept, 0)

    def finish_first(i, c):
        first(lax.rem(t + i, n_tm)).wait_send()
        return c

    lax.fori_loop(1, n_tm, finish_first, 0)

    def finish_group(k, c):
        other = lax.rem(f + k, n_fq)

        def finish(s, c):
            second(other, s).wait_send()
            second_landed(other, s).wait_recv()
            return c

        return lax.fori_loop(0, span, finish, c)

    lax.fori_loop(1, n_fq, finish_group, 0)


def exchange(strengths, halo_cols, table, select, n_tm, n_fq):
    parts, groups, channels, samples = strengths.shape
    span = n_tm // n_fq
    chunk = channels // n_tm
    block = (SLABS, parts * groups * chunk, FFT_HI)
    return pl.pallas_call(
        functools.partial(exchange_kernel, n_tm, n_fq),
        out_shape=jax.ShapeDtypeStruct((2 * n_fq, span) + block, jnp.bfloat16),
        in_specs=[pl.BlockSpec(memory_space=pl.ANY)] + [pl.BlockSpec(memory_space=pltpu.VMEM)] * 3,
        out_specs=pl.BlockSpec(memory_space=pl.ANY),
        scratch_shapes=[
            pltpu.VMEM((n_tm, parts, groups, chunk, samples), jnp.bfloat16),
            pltpu.VMEM((n_tm,) + block, jnp.bfloat16),
            pltpu.SemaphoreType.DMA((n_tm,)),
            pltpu.SemaphoreType.DMA((n_tm,)),
            pltpu.SemaphoreType.DMA((n_tm,)),
            pltpu.SemaphoreType.DMA((n_fq, span)),
            pltpu.SemaphoreType.DMA((n_fq, span)),
            pltpu.SemaphoreType.DMA,
        ],
        compiler_params=pltpu.CompilerParams(
            collective_id=0, has_side_effects=True, vmem_limit_bytes=48 * 1024 * 1024
        ),
        name="spread_exchange",
    )(strengths, halo_cols, table, select)


def fft_list(re, im):
    n = len(re)
    if n == 1:
        return re, im
    er, ei = fft_list(re[0::2], im[0::2])
    orr, oi = fft_list(re[1::2], im[1::2])
    out_r, out_i = [None] * n, [None] * n
    for k in range(n // 2):
        c, s = math.cos(2 * math.pi * k / n), math.sin(2 * math.pi * k / n)
        a, b = orr[k], oi[k]
        if k == 0:
            tr, ti = a, b
        elif 4 * k == n:
            tr, ti = b, -a
        elif 8 * k == n:
            tr, ti = (a + b) * c, (b - a) * c
        elif 8 * k == 3 * n:
            tr, ti = (b - a) * s, -(a + b) * s
        else:
            tr, ti = a * c + b * s, b * c - a * s
        out_r[k], out_i[k] = er[k] + tr, ei[k] + ti
        out_r[k + n // 2], out_i[k + n // 2] = er[k] - tr, ei[k] - ti
    return out_r, out_i


def transform_kernel(x_ref, tc_ref, ts_ref, hi_ref, o_ref, lhs):
    chunk = x_ref.shape[5]
    re = [x_ref[0, n // SLABS, n % SLABS, 0, 0].astype(jnp.float32) for n in range(FFT_LO)]
    im = [x_ref[0, n // SLABS, n % SLABS, 1, 0].astype(jnp.float32) for n in range(FFT_LO)]
    re, im = fft_list(re, im)
    for a in range(FFT_LO):
        c = tc_ref[a : a + 1, :]
        s = ts_ref[a : a + 1, :]
        rows = pl.ds(a * chunk, chunk)
        lhs[rows, :FFT_HI] = (re[a] * c + im[a] * s).astype(jnp.bfloat16)
        lhs[rows, FFT_HI:] = (im[a] * c - re[a] * s).astype(jnp.bfloat16)
    x = lhs[...]
    y = jnp.dot(x, hi_ref[...], preferred_element_type=jnp.float32)
    flat = o_ref.reshape(2, chunk * FFT_LO, FFT_HI)
    for a in range(FFT_LO):
        for p in range(2):
            flat[p, pl.ds(a, chunk, stride=FFT_LO), :] = y[
                a * chunk : (a + 1) * chunk, p * FFT_HI : (p + 1) * FFT_HI
            ]


def transform(held, n_fq, groups, chunk, frames):
    span = held.shape[1]
    x = held.reshape(2 * n_fq, span, SLABS, 2, groups, chunk, FFT_HI)
    low = np.arange(FFT_LO)[:, None] * np.arange(FFT_HI)[None, :] * (2 * math.pi / FFTLEN)
    high = np.arange(FFT_HI)[:, None] * np.arange(FFT_HI)[None, :] % FFT_HI * (2 * math.pi / FFT_HI)
    hc, hs = np.cos(high), np.sin(high)
    full = np.block([[hc, -hs], [hs, hc]]).astype(np.float32) / math.sqrt(FFTLEN)
    hi = full.astype(jnp.bfloat16)
    whole = lambda shape: pl.BlockSpec(shape, lambda f, g, m: (0, 0))
    return pl.pallas_call(
        transform_kernel,
        out_shape=jax.ShapeDtypeStruct(
            (2, n_fq * groups, chunk, frames, FFT_LO, FFT_HI), jnp.float32
        ),
        grid=(n_fq, groups, frames),
        in_specs=[
            pl.BlockSpec(
                (1, PER_FRAME, SLABS, 2, 1, chunk, FFT_HI), lambda f, g, m: (f, m, 0, 0, g, 0, 0)
            ),
            whole((FFT_LO, FFT_HI)),
            whole((FFT_LO, FFT_HI)),
            whole((2 * FFT_HI, 2 * FFT_HI)),
        ],
        out_specs=pl.BlockSpec(
            (2, 1, chunk, 1, FFT_LO, FFT_HI), lambda f, g, m: (0, f * groups + g, 0, m, 0, 0)
        ),
        scratch_shapes=[
            pltpu.VMEM((FFT_LO * chunk, 2 * FFT_HI), jnp.bfloat16),
        ],
        name="transform",
    )(
        x,
        jnp.asarray(np.cos(low), jnp.float32),
        jnp.asarray(np.sin(low), jnp.float32),
        jnp.asarray(hi),
    )


def shards(strengths, sample_cell, sample_frac):
    n_tm, n_fq = lax.axis_size("tm"), lax.axis_size("freq")
    parts, groups, channels, samples = strengths.shape
    local_cell = sample_cell - lax.axis_index("tm") * GRID_DEV
    edge_columns = jnp.concatenate(
        [
            jnp.arange(HALF, dtype=jnp.int32),
            jnp.arange(GRID_DEV + HALF, GRID_DEV + TAPS, dtype=jnp.int32),
        ]
    )
    edge_table = tap_table(local_cell, sample_frac, edge_columns)
    edges = lax.dot_general(
        edge_table,
        strengths.reshape(parts * groups * channels, samples),
        (((0,), (1,)), ((), ())),
        preferred_element_type=jnp.float32,
    )
    from_left = lax.ppermute(edges[HALF:], "tm", [(i, (i + 1) % n_tm) for i in range(n_tm)])
    from_right = lax.ppermute(edges[:HALF], "tm", [((i + 1) % n_tm, i) for i in range(n_tm)])
    table = tap_table(local_cell, sample_frac, jnp.arange(HALF, HALF + GRID_DEV, dtype=jnp.int32))
    halo = jnp.concatenate([from_left, from_right], axis=0)
    h0 = lax.reduce_precision(halo, 8, 7)
    h1 = lax.reduce_precision(halo - h0, 8, 7)
    h2 = halo - h0 - h1
    split = jnp.concatenate([h0, h1, h2], axis=0)
    halo_cols = jnp.pad(split.T, ((0, 0), (0, 128 - 3 * TAPS))).astype(jnp.bfloat16)
    pick = np.zeros((128, GRID_DEV), np.float32)
    for r in range(3):
        for k in range(HALF):
            pick[r * TAPS + k, k] = 1.0
            pick[r * TAPS + HALF + k, GRID_DEV - HALF + k] = 1.0
    held = exchange(
        strengths,
        halo_cols.reshape(parts, groups, channels, 128),
        table,
        jnp.asarray(pick, jnp.bfloat16),
        n_tm,
        n_fq,
    )
    frames = n_tm // PER_FRAME // n_fq
    return transform(held, n_fq, groups, channels // n_tm, frames)


def solution(mesh):
    placed = (P(None, "freq", None, "tm"), P("tm"), P("tm"))
    return jax.shard_map(
        shards,
        mesh=mesh,
        in_specs=placed,
        out_specs=P(None, None, "tm", "freq", None, None),
        check_vma=False,
    )
```

```python
import functools
import math

import jax
import jax.numpy as jnp
import numpy as np
from jax import lax
from jax.experimental import pallas as pl
from jax.experimental.pallas import tpu as pltpu
from jax.sharding import PartitionSpec as P

TAPS = 8
HALF = TAPS // 2
GRID_DEV = 1024
FFT_LO = 32
FFT_HI = 128
FFTLEN = 4096
SHARP = 0.3
MESH = pl.DeviceIdType.MESH
SLABS = GRID_DEV // FFT_HI
PER_FRAME = FFTLEN // GRID_DEV


def tap_table(local_cell, fraction, columns):
    offset = columns[None, :] - local_cell[:, None] - 1
    inside = (offset >= 0) & (offset < TAPS)
    shifted = offset.astype(jnp.float32) - float(HALF - 1) - fraction[:, None]
    values = jnp.exp(-SHARP * (shifted * shifted))
    return jnp.where(inside, values, 0.0).astype(jnp.bfloat16)


def exchange_kernel(
    n_tm, n_fq, strengths, halo, table, select, out, held, src, load, send1, recv1, send2, recv2, local_sem
):
    t = lax.axis_index("tm")
    f = lax.axis_index("freq")
    span = n_tm // n_fq
    slot = lax.rem(t, span)
    home = lax.div(t, span)
    barrier = pltpu.get_barrier_semaphore()

    def greet_tm(i, c):
        pl.semaphore_signal(barrier, inc=1, device_id=(lax.rem(t + i, n_tm), f), device_id_type=MESH)
        return c

    def greet_fq(i, c):
        pl.semaphore_signal(barrier, inc=1, device_id=(t, lax.rem(f + i, n_fq)), device_id_type=MESH)
        return c

    lax.fori_loop(1, n_tm, greet_tm, 0)
    lax.fori_loop(1, n_fq, greet_fq, 0)
    half = n_tm // 2
    upper = lax.div(t, half)
    quarter = lax.div(t, half // 2)
    outer = lax.rem(lax.div(quarter + 1, 2) + 1, 2)
    chunk = held.shape[3]
    rows = src.shape[2]

    def dest(i):
        side = lax.rem(lax.div(i, half) + 1 + outer + upper, 2)
        return side * half + lax.rem(t + half // 2 + i, half)

    def fetch(i):
        channels = pl.ds(pl.multiple_of(dest(i) * chunk, chunk), chunk)
        return pltpu.make_async_copy(strengths.at[:, :, channels, :], held.at[i], load.at[i])

    def fetch_one(i, c):
        fetch(i).start()
        return c

    lax.fori_loop(0, n_tm, fetch_one, 0)

    def make(i):
        fetch(i).wait()
        channels = pl.ds(pl.multiple_of(dest(i) * chunk, chunk), chunk)
        x = held[i].reshape(rows, held.shape[4])
        h = halo[:, :, channels, :].reshape(rows, halo.shape[3])
        acc = jnp.dot(x, table[...], preferred_element_type=jnp.float32)
        acc = acc + jnp.dot(h, select[...], preferred_element_type=jnp.float32)
        acc = acc.astype(jnp.bfloat16)
        for j in range(SLABS):
            src[dest(i), j] = acc[:, j * FFT_HI : (j + 1) * FFT_HI]

    make(0)
    pl.semaphore_wait(barrier, n_tm - 1 + n_fq - 1)

    def place(target):
        return jnp.where(target == f, f, n_fq + target)

    def first(peer):
        return pltpu.make_async_remote_copy(
            src_ref=src.at[peer],
            dst_ref=out.at[place(home), slot],
            send_sem=send1.at[peer],
            recv_sem=recv1.at[t],
            device_id=(peer, f),
            device_id_type=MESH,
        )

    def first_landed(origin):
        return pltpu.make_async_remote_copy(
            src_ref=src.at[origin],
            dst_ref=out.at[place(lax.div(origin, span)), lax.rem(origin, span)],
            send_sem=send1.at[origin],
            recv_sem=recv1.at[origin],
            device_id=(origin, f),
            device_id_type=MESH,
        )

    def second(target, s):
        return pltpu.make_async_remote_copy(
            src_ref=out.at[n_fq + target, s],
            dst_ref=out.at[f, s],
            send_sem=send2.at[target, s],
            recv_sem=recv2.at[f, s],
            device_id=(t, target),
            device_id_type=MESH,
        )

    def second_landed(origin, s):
        return pltpu.make_async_remote_copy(
            src_ref=out.at[n_fq + origin, s],
            dst_ref=out.at[origin, s],
            send_sem=send2.at[origin, s],
            recv_sem=recv2.at[origin, s],
            device_id=(t, origin),
            device_id_type=MESH,
        )

    def step(i, c):
        make(i)
        send(i - 1)
        return c

    def send(i):
        peer = dest(i)

        @pl.when(peer != t)
        def _():
            first(peer).start()

    lax.fori_loop(1, n_tm, step, 0)
    own = pltpu.make_async_copy(src.at[t], out.at[place(home), slot], local_sem)
    own.start()
    own.wait()
    send(n_tm - 1)

    def relay_group(k, c):
        target = lax.rem(f + k, n_fq)

        def relay(i, c):
            part = span // 2
            s = lax.rem(lax.div(i, part) + upper, 2) * part + lax.rem(slot + 2 * span - i, part)
            origin = target * span + s

            @pl.when(origin != t)
            def _():
                first_landed(origin).wait_recv()

            second(target, s).start()
            return c

        return lax.fori_loop(0, span, relay, c)

    lax.fori_loop(1, n_fq, relay_group, 0)

    def kept(s, c):
        origin = f * span + s

        @pl.when(origin != t)
        def _():
            first_landed(origin).wait_recv()

        return c

    lax.fori_loop(0, span, kept, 0)

    def finish_first(i, c):
        first(lax.rem(t + i, n_tm)).wait_send()
        return c

    lax.fori_loop(1, n_tm, finish_first, 0)

    def finish_group(k, c):
        other = lax.rem(f + k, n_fq)

        def finish(s, c):
            second(other, s).wait_send()
            second_landed(other, s).wait_recv()
            return c

        return lax.fori_loop(0, span, finish, c)

    lax.fori_loop(1, n_fq, finish_group, 0)


def exchange(strengths, halo_cols, table, select, n_tm, n_fq):
    parts, groups, channels, samples = strengths.shape
    span = n_tm // n_fq
    chunk = channels // n_tm
    block = (SLABS, parts * groups * chunk, FFT_HI)
    return pl.pallas_call(
        functools.partial(exchange_kernel, n_tm, n_fq),
        out_shape=jax.ShapeDtypeStruct((2 * n_fq, span) + block, jnp.bfloat16),
        in_specs=[pl.BlockSpec(memory_space=pl.ANY)] + [pl.BlockSpec(memory_space=pltpu.VMEM)] * 3,
        out_specs=pl.BlockSpec(memory_space=pl.ANY),
        scratch_shapes=[
            pltpu.VMEM((n_tm, parts, groups, chunk, samples), jnp.bfloat16),
            pltpu.VMEM((n_tm,) + block, jnp.bfloat16),
            pltpu.SemaphoreType.DMA((n_tm,)),
            pltpu.SemaphoreType.DMA((n_tm,)),
            pltpu.SemaphoreType.DMA((n_tm,)),
            pltpu.SemaphoreType.DMA((n_fq, span)),
            pltpu.SemaphoreType.DMA((n_fq, span)),
            pltpu.SemaphoreType.DMA,
        ],
        compiler_params=pltpu.CompilerParams(
            collective_id=0, has_side_effects=True, vmem_limit_bytes=48 * 1024 * 1024
        ),
        name="spread_exchange",
    )(strengths, halo_cols, table, select)


def fft_list(re, im):
    n = len(re)
    if n == 1:
        return re, im
    er, ei = fft_list(re[0::2], im[0::2])
    orr, oi = fft_list(re[1::2], im[1::2])
    out_r, out_i = [None] * n, [None] * n
    for k in range(n // 2):
        c, s = math.cos(2 * math.pi * k / n), math.sin(2 * math.pi * k / n)
        a, b = orr[k], oi[k]
        if k == 0:
            tr, ti = a, b
        elif 4 * k == n:
            tr, ti = b, -a
        elif 8 * k == n:
            tr, ti = (a + b) * c, (b - a) * c
        elif 8 * k == 3 * n:
            tr, ti = (b - a) * s, -(a + b) * s
        else:
            tr, ti = a * c + b * s, b * c - a * s
        out_r[k], out_i[k] = er[k] + tr, ei[k] + ti
        out_r[k + n // 2], out_i[k + n // 2] = er[k] - tr, ei[k] - ti
    return out_r, out_i


def transform_kernel(x_ref, tc_ref, ts_ref, hi_ref, o_ref, lhs):
    chunk = x_ref.shape[5]
    re = [x_ref[0, n // SLABS, n % SLABS, 0, 0].astype(jnp.float32) for n in range(FFT_LO)]
    im = [x_ref[0, n // SLABS, n % SLABS, 1, 0].astype(jnp.float32) for n in range(FFT_LO)]
    re, im = fft_list(re, im)
    for a in range(FFT_LO):
        c = tc_ref[a : a + 1, :]
        s = ts_ref[a : a + 1, :]
        rows = pl.ds(a * chunk, chunk)
        lhs[rows, :FFT_HI] = (re[a] * c + im[a] * s).astype(jnp.bfloat16)
        lhs[rows, FFT_HI:] = (im[a] * c - re[a] * s).astype(jnp.bfloat16)
    x = lhs[...]
    y = jnp.dot(x, hi_ref[...], preferred_element_type=jnp.float32)
    flat = o_ref.reshape(2, chunk * FFT_LO, FFT_HI)
    for a in range(FFT_LO):
        for p in range(2):
            flat[p, pl.ds(a, chunk, stride=FFT_LO), :] = y[
                a * chunk : (a + 1) * chunk, p * FFT_HI : (p + 1) * FFT_HI
            ]


def transform(held, n_fq, groups, chunk, frames):
    span = held.shape[1]
    x = held.reshape(2 * n_fq, span, SLABS, 2, groups, chunk, FFT_HI)
    low = np.arange(FFT_LO)[:, None] * np.arange(FFT_HI)[None, :] * (2 * math.pi / FFTLEN)
    high = np.arange(FFT_HI)[:, None] * np.arange(FFT_HI)[None, :] % FFT_HI * (2 * math.pi / FFT_HI)
    hc, hs = np.cos(high), np.sin(high)
    full = np.block([[hc, -hs], [hs, hc]]).astype(np.float32) / math.sqrt(FFTLEN)
    hi = full.astype(jnp.bfloat16)
    whole = lambda shape: pl.BlockSpec(shape, lambda f, g, m: (0, 0))
    return pl.pallas_call(
        transform_kernel,
        out_shape=jax.ShapeDtypeStruct(
            (2, n_fq * groups, chunk, frames, FFT_LO, FFT_HI), jnp.float32
        ),
        grid=(n_fq, groups, frames),
        in_specs=[
            pl.BlockSpec(
                (1, PER_FRAME, SLABS, 2, 1, chunk, FFT_HI), lambda f, g, m: (f, m, 0, 0, g, 0, 0)
            ),
            whole((FFT_LO, FFT_HI)),
            whole((FFT_LO, FFT_HI)),
            whole((2 * FFT_HI, 2 * FFT_HI)),
        ],
        out_specs=pl.BlockSpec(
            (2, 1, chunk, 1, FFT_LO, FFT_HI), lambda f, g, m: (0, f * groups + g, 0, m, 0, 0)
        ),
        scratch_shapes=[
            pltpu.VMEM((FFT_LO * chunk, 2 * FFT_HI), jnp.bfloat16),
        ],
        name="transform",
    )(
        x,
        jnp.asarray(np.cos(low), jnp.float32),
        jnp.asarray(np.sin(low), jnp.float32),
        jnp.asarray(hi),
    )


def shards(strengths, sample_cell, sample_frac):
    n_tm, n_fq = lax.axis_size("tm"), lax.axis_size("freq")
    parts, groups, channels, samples = strengths.shape
    local_cell = sample_cell - lax.axis_index("tm") * GRID_DEV
    edge_columns = jnp.concatenate(
        [
            jnp.arange(HALF, dtype=jnp.int32),
            jnp.arange(GRID_DEV + HALF, GRID_DEV + TAPS, dtype=jnp.int32),
        ]
    )
    edge_table = tap_table(local_cell, sample_frac, edge_columns)
    edges = lax.dot_general(
        edge_table,
        strengths.reshape(parts * groups * channels, samples),
        (((0,), (1,)), ((), ())),
        preferred_element_type=jnp.float32,
    )
    from_left = lax.ppermute(edges[HALF:], "tm", [(i, (i + 1) % n_tm) for i in range(n_tm)])
    from_right = lax.ppermute(edges[:HALF], "tm", [((i + 1) % n_tm, i) for i in range(n_tm)])
    table = tap_table(local_cell, sample_frac, jnp.arange(HALF, HALF + GRID_DEV, dtype=jnp.int32))
    halo = jnp.concatenate([from_left, from_right], axis=0)
    h0 = lax.reduce_precision(halo, 8, 7)
    h1 = lax.reduce_precision(halo - h0, 8, 7)
    h2 = halo - h0 - h1
    split = jnp.concatenate([h0, h1, h2], axis=0)
    halo_cols = jnp.pad(split.T, ((0, 0), (0, 128 - 3 * TAPS))).astype(jnp.bfloat16)
    pick = np.zeros((128, GRID_DEV), np.float32)
    for r in range(3):
        for k in range(HALF):
            pick[r * TAPS + k, k] = 1.0
            pick[r * TAPS + HALF + k, GRID_DEV - HALF + k] = 1.0
    held = exchange(
        strengths,
        halo_cols.reshape(parts, groups, channels, 128),
        table,
        jnp.asarray(pick, jnp.bfloat16),
        n_tm,
        n_fq,
    )
    frames = n_tm // PER_FRAME // n_fq
    return transform(held, n_fq, groups, channels // n_tm, frames)


def solution(mesh):
    placed = (P(None, "freq", None, "tm"), P("tm"), P("tm"))
    return jax.shard_map(
        shards,
        mesh=mesh,
        in_specs=placed,
        out_specs=P(None, None, "tm", "freq", None, None),
        check_vma=False,
    )
```
